32 devices in a mesh: rel: 4 (over x, core), dst: 4 (over z), mp: 2 (over y).
Axes of the slice: x: 2, y: 2, z: 4, core: 2. Of those that a mesh axis runs over, the one named last changes fastest.
Arguments:
- node_table: bfloat16 [16384, 512], P(('rel', 'dst')), may hold values from -6 to 6
- edge_weights: bfloat16 [4, 32, 128, 128], P('rel', 'dst'), may hold values from -0.5 to 0.5
- src_ids: int32 [4, 32, 128], P('rel', 'dst'), may hold values from 0 to 1023
- dst_ids: int32 [4, 32, 128], P('rel', 'dst'), may hold values from 0 to 511
- block_mask: int32 [4, 32], P('rel', 'dst'), may hold values 0 or 1
- basis_coef: float32 [4, 32], P('rel'), may hold values from -0.375 to 0.375
- basis_mats: bfloat16 [32, 512, 512], P(None, None, 'mp'), may hold values from -0.25 to 0.25
- type_bias: float32 [4, 512], P(None, 'mp'), may hold values from -3 to 3
- type_rows: int32 [4], replicated, may hold values from 1 to 256, 512 in all
- cotangent: bfloat16 [2048, 512], P(('rel', 'dst'), 'mp'), may hold values from -0.005859375 to 0.005859375
Outputs:
- layer_out: bfloat16 [2048, 512], P(('rel', 'dst'), 'mp')
- coef_grad: float32 [4, 32], P('rel')
The draws below stay inside these ranges and needn't reach their ends.
Inputs may be any that keep to these rules, and one draw needn't show every extreme that they name: `type_rows`: the 4 counts sum to 512.
All inputs are finite; a program needn't handle non-finite values. No bound on the sum of `block_mask` on one device may be relied on, other than what follows from the above.
Results may differ from the reference program's by a relative error of at most 0.0062.
Values may be sent and summed in bfloat16 or wider, within the bound.
No kernel may reach another device: no remote copies, remote signals or barrier semaphores. Data moves between devices by JAX's collectives and lax.ppermute only.
A program may use at most 64 MiB of HBM per device.

```python
import math
import jax
import jax.numpy as jnp
import numpy as np
from jax import lax

F = 512
BASES = 32
BLK = 128
TYPES = 4
BPO = 2
ROWS_DEV = 128
TAB_DEV = 1024
RELATIONS = 4
NBLK = 8
OWN = 512
TABLE = 16384
OUTROWS = 2048
N_REL = 4
N_DST = 4


def plant(result, stream_key, least, high):
    place = [jax.random.randint(jax.random.fold_in(stream_key, axis), (), 0, length) for axis, length in enumerate(result.shape)]
    widest = result.shape.index(max(result.shape))
    neighbour = place[:widest] + [(place[widest] + 1) % result.shape[widest]] + place[widest + 1:]
    return result.at[tuple(place)].set(least).at[tuple(neighbour)].set(high)


def shard_levels(rng, extent, cuts, smallest, largest):
    level, own = 1.0, jax.random.fold_in(rng, 6)
    for dim, parts in cuts:
        steps = jnp.exp(jax.random.uniform(jax.random.fold_in(own, dim), (parts,), jnp.float32, smallest / len(cuts), largest / len(cuts)))
        level = level * jnp.repeat(steps, extent[dim] // parts).reshape([-1 if axis == dim else 1 for axis in range(len(extent))])
    return level


def split_up(amount, total, most, lean):
    loads = [(1 << 20) // math.isqrt(grade ** lean) + 1 for grade in range(2, amount + 1)]
    spare, holding = total - most - (amount - 1), [1] * (amount - 1)
    while spare > 0:
        free = [i for i in range(amount - 1) if holding[i] < most]
        whole, budget = sum([loads[i] for i in free]), spare
        for i in free:
            extra = min(most - holding[i], max(1, budget * loads[i] // whole), spare)
            holding[i] = holding[i] + extra
            spare = spare - extra
    return np.array([most] + holding)


def ragged(stream_key, number_of, total, limit, lean):
    if number_of == 2:
        one = jax.random.randint(stream_key, (), max(1, total - limit), min(limit, total - 1) + 1)
        return jnp.stack([one, total - one])
    sizes = jnp.asarray(split_up(number_of, total, limit, lean), jnp.int32)
    couples = (number_of - 1) // 2
    giver, receiver = sizes[1:1 + 2 * couples:2], sizes[2:2 + 2 * couples:2]
    margin = jnp.minimum(giver - 1, limit - receiver)
    moved = jax.random.randint(jax.random.fold_in(stream_key, 1), (couples,), 0, 1 << 20) % (margin + 1)
    sizes = sizes.at[1:1 + 2 * couples:2].set(giver - moved).at[2:2 + 2 * couples:2].set(receiver + moved)
    return sizes[jax.random.permutation(jax.random.fold_in(stream_key, 2), number_of)]


def scatter_about(own_key, shape, spread, most, cuts=(), kind=jnp.bfloat16):
    drawn = spread * jax.random.normal(own_key, shape, jnp.float32)
    if cuts:
        drawn = drawn * shard_levels(own_key, shape, cuts, -0.22, 0.18)
    return jnp.clip(drawn, -most, most).astype(kind)


def setup_inputs(seed: int = 0) -> dict:
    splits = jax.random.split(jax.random.key(seed), 11)
    return {
        "node_table": scatter_about(splits[0], (TABLE, F), 1.0, 6.0, ((0, 16),)),
        "edge_weights": scatter_about(splits[1], (RELATIONS, N_DST * NBLK, BLK, BLK), BLK ** -0.5, 0.5, ((0, 4), (1, 4))),
        "src_ids": plant(jax.random.randint(splits[2], (RELATIONS, N_DST * NBLK, BLK), 0, TAB_DEV), jax.random.fold_in(splits[2], 1), 0, TAB_DEV - 1).astype(jnp.int32),
        "dst_ids": plant(jax.random.randint(splits[3], (RELATIONS, N_DST * NBLK, BLK), 0, OWN), jax.random.fold_in(splits[3], 1), 0, OWN - 1).astype(jnp.int32),
        "block_mask": plant((jax.random.randint(splits[4], (RELATIONS, N_DST * NBLK), 0, 3) < 2).astype(jnp.int32), jax.random.fold_in(splits[4], 1), 0, 1),
        "basis_coef": scatter_about(splits[5], (RELATIONS, BASES), (BASES * NBLK * BLK // ROWS_DEV) ** -0.5, 0.375, ((0, 4),), jnp.float32),
        "basis_mats": scatter_about(splits[6], (BASES, F, F), F ** -0.5, 0.25, ((2, 2),)),
        "type_bias": scatter_about(splits[7], (TYPES, F), 0.5, 3.0, ((1, 2),), jnp.float32),
        "type_rows": ragged(splits[8], TYPES, OWN, OWN // 2, 2).astype(jnp.int32),
        "cotangent": scatter_about(splits[9], (OUTROWS, F), (N_DST * NBLK * BLK * F // 2) ** -0.5, 0.005859375, ((0, 16), (1, 2))),
    }


highest = lax.Precision.HIGHEST


def reference(node_table, edge_weights, src_ids, dst_ids, block_mask, basis_coef, basis_mats, type_bias, type_rows, cotangent):
    features = node_table.shape[1]
    owner_span = ROWS_DEV * N_REL
    basis_full = basis_mats.astype(jnp.float32)
    mixing = jnp.einsum('rb,bfg->rfg', basis_coef, basis_full, precision=highest).astype(jnp.bfloat16)
    owner_grad = cotangent.reshape(N_REL, N_DST, ROWS_DEV, features).transpose(1, 0, 2, 3).reshape(N_DST, owner_span, features)
    owners = jnp.arange(NBLK, dtype=jnp.int32) // BPO
    owner_rows = jnp.broadcast_to(owners[:, None], (NBLK, BLK)).reshape(-1)

    def visit(state_pair, pair_index):
        summed, basis_grads = state_pair
        relation = pair_index // N_DST
        source = pair_index % N_DST
        zero = jnp.zeros((), jnp.int32)
        table_rows = lax.dynamic_slice_in_dim(node_table, ((relation * N_DST + source) * TAB_DEV).astype(jnp.int32), TAB_DEV, 0)
        start = (source * NBLK).astype(jnp.int32)
        source_ids = lax.dynamic_slice(src_ids, (relation, start, zero), (1, NBLK, BLK))[0]
        slot_ids = lax.dynamic_slice(dst_ids, (relation, start, zero), (1, NBLK, BLK))[0].reshape(-1)
        blocks = lax.dynamic_slice(edge_weights, (relation, start, zero, zero), (1, NBLK, BLK, BLK))[0].astype(jnp.float32)
        live_blocks = lax.dynamic_slice(block_mask, (relation, start), (1, NBLK))[0].astype(jnp.float32)
        picked = table_rows[source_ids.reshape(-1)].reshape(NBLK, BLK, features).astype(jnp.float32)
        messages = jnp.einsum('kij,kjf->kif', blocks * live_blocks[:, None, None], picked, precision=highest)
        messages = messages.astype(jnp.bfloat16).reshape(-1, features).astype(jnp.float32)
        weight = mixing[relation].astype(jnp.float32)
        outgoing = jnp.dot(messages, weight, precision=highest).astype(jnp.bfloat16)
        summed = summed.at[owner_rows, slot_ids].add(outgoing.astype(jnp.float32))
        wanted = owner_grad[owner_rows, slot_ids].astype(jnp.float32)
        outer_sum = jnp.dot(messages.T, wanted, precision=highest)
        update = jnp.einsum('bfg,fg->b', basis_full, outer_sum, precision=highest)
        basis_grads = basis_grads.at[relation].add(update)
        return (summed, basis_grads), None

    start_state = (jnp.zeros((N_DST, owner_span, features), jnp.float32), jnp.zeros((N_REL, BASES), jnp.float32))
    (summed, basis_grads), _ = lax.scan(visit, start_state, jnp.arange(N_REL * N_DST, dtype=jnp.int32))
    bounds = jnp.cumsum(type_rows)
    position = jnp.arange(owner_span, dtype=jnp.int32)
    row_kind = jnp.minimum(jnp.sum((position[:, None] >= bounds[None, :]).astype(jnp.int32), axis=1), TYPES - 1)
    row_bias = type_bias[row_kind]
    layer_out = (summed + row_bias[None]).reshape(N_DST, N_REL, ROWS_DEV, features).transpose(1, 0, 2, 3)
    layer_out = layer_out.reshape(-1, features).astype(jnp.bfloat16)
    return layer_out, basis_grads
```

```python
import functools
import jax
import jax.numpy as jnp
from jax import lax
from jax.experimental import pallas as pl
from jax.experimental.pallas import tpu as pltpu
from jax.sharding import PartitionSpec as P

f32, bf16, i32 = jnp.float32, jnp.bfloat16, jnp.int32
LIMIT = 40 * 1024 * 1024
CONTRACT_ROWS = (((0,), (0,)), ((), ()))


def whole(space=pltpu.VMEM):
    return pl.BlockSpec(memory_space=space)


def swap(x, axis, d):
    n = lax.axis_size(axis)
    return lax.ppermute(x, axis, [(i, i ^ d) for i in range(n)])


def spread_rows(row, rows):
    return jnp.broadcast_to(row, (rows, rows)).T


def one_hot(column, width):
    rows, lanes = column.shape
    lane = lax.broadcasted_iota(i32, (rows, lanes), 1)
    parts = [(column == lane + c).astype(bf16) for c in range(0, width, lanes)]
    return jnp.concatenate(parts, axis=1)


def send_kernel(
    n_dst, coef, mask, src, dst, table, weights, basis, messages, *rest
):
    outs, acc = rest[:n_dst], rest[n_dst]
    step, steps = pl.program_id(0), pl.num_programs(0)
    per_step, features, cols = basis.shape
    block = weights.shape[-1]
    blocks = src.shape[1]
    per_owner = blocks // n_dst

    column = spread_rows(src[0, pl.ds(step, 1), :], block)
    picked = jnp.dot(
        one_hot(column, table.shape[0]), table[...], preferred_element_type=f32
    ).astype(bf16)
    scaled = weights[0, 0] * mask[0, step].astype(f32).astype(bf16)
    rows = pl.ds(pl.multiple_of(step * block, block), block)
    messages[rows, :] = jnp.dot(scaled, picked, preferred_element_type=f32).astype(bf16)

    factors = [coef[0, step * per_step + b] for b in range(per_step)]
    chunk = 64
    for start in range(0, features, chunk):
        part = pl.ds(start, chunk)
        total = factors[0] * basis[0, part, :].astype(f32)
        for b in range(1, per_step):
            total = total + factors[b] * basis[b, part, :].astype(f32)

        @pl.when(step == 0)
        def _():
            acc[part, :] = total

        @pl.when(step > 0)
        def _():
            acc[part, :] = acc[part, :] + total

    @pl.when(step == steps - 1)
    def _():
        weight = acc[...].astype(bf16)
        me = lax.axis_index("dst")
        span = per_owner * block
        for d in range(n_dst):
            owner = me ^ d
            mine = messages[pl.ds(pl.multiple_of(owner * span, span), span), :]
            outs[d][:span, :] = jnp.dot(mine, weight, preferred_element_type=f32).astype(bf16)
            pad = outs[d].shape[0] - span
            which = lax.broadcasted_iota(i32, (pad, block), 0)
            slots = jnp.zeros((pad, block), i32)
            for b in range(per_owner):
                ids = dst[0, pl.ds(owner * per_owner + b, 1), :]
                slots = jnp.where(which == 2 * b, ids & 255, slots)
                slots = jnp.where(which == 2 * b + 1, ids >> 8, slots)
            outs[d][span:, :block] = slots.astype(f32).astype(bf16)
            outs[d][span:, block:] = jnp.zeros((pad, cols - block), bf16)


def send(coef, mask, src, dst, table, weights, basis, n_dst):
    count, features, cols = basis.shape
    blocks, block = src.shape[1:]
    per_step = count // blocks
    span = blocks // n_dst * block
    pad = -(-2 * (blocks // n_dst) // 16) * 16
    smem = pl.BlockSpec(memory_space=pltpu.SMEM)
    return pl.pallas_call(
        functools.partial(send_kernel, n_dst),
        grid=(blocks,),
        in_specs=[
            smem,
            smem,
            whole(),
            whole(),
            whole(),
            pl.BlockSpec((1, 1, block, block), lambda k: (0, k, 0, 0)),
            pl.BlockSpec((per_step, features, cols), lambda k: (k, 0, 0)),
        ],
        out_shape=[jax.ShapeDtypeStruct((blocks * block, features), bf16)]
        + [jax.ShapeDtypeStruct((span + pad, cols), bf16)] * n_dst,
        out_specs=[whole()] * (1 + n_dst),
        scratch_shapes=[pltpu.VMEM((features, cols), f32)],
        compiler_params=pltpu.CompilerParams(
            dimension_semantics=("arbitrary",), vmem_limit_bytes=LIMIT
        ),
        cost_estimate=pl.CostEstimate(flops=6_000_000_000, bytes_accessed=10_000_000, transcendentals=0),
        name="send",
    )(coef, mask, src, dst, table, weights, basis)


def grad_kernel(n_rel, n_dst, dst, messages, basis, *rest):
    pieces, out = rest[: n_rel * n_dst], rest[n_rel * n_dst]
    table, outer, sums = rest[n_rel * n_dst + 1 :]
    step, steps = pl.program_id(0), pl.num_programs(0)
    per_step, features, cols = basis.shape
    blocks, block = dst.shape[1:]
    rows_dev = pieces[0].shape[0]
    per_owner = blocks // n_dst
    span = per_owner * block
    owner_rows = n_rel * rows_dev

    @pl.when(step == 0)
    def _():
        rel, me = lax.axis_index("rel"), lax.axis_index("dst")
        for d in range(n_dst):
            for e in range(n_rel):
                at = (me ^ d) * owner_rows + (rel ^ e) * rows_dev
                table[pl.ds(pl.multiple_of(at, rows_dev), rows_dev), :] = pieces[
                    d * n_rel + e
                ][...]
        total = jnp.zeros((features, cols), f32)
        for o in range(n_dst):
            own = table[o * owner_rows : (o + 1) * owner_rows, :]
            parts = []
            for b in range(per_owner):
                k = o * per_owner + b
                column = spread_rows(dst[0, k : k + 1, :], block)
                parts.append(one_hot(column, owner_rows))
            picks = jnp.concatenate(parts, axis=0)
            wanted = jnp.dot(picks, own, preferred_element_type=f32).astype(bf16)
            total = total + lax.dot_general(
                messages[o * span : (o + 1) * span, :],
                wanted,
                CONTRACT_ROWS,
                preferred_element_type=f32,
            )
        outer[...] = total

    for b in range(per_step):
        total = jnp.zeros((8, 128), f32)
        for start in range(0, features, 32):
            part = pl.ds(start, 32)
            prod = basis[b, part, :].astype(f32) * outer[part, :]
            for r in range(0, 32, 8):
                for c in range(0, cols, 128):
                    total = total + prod[r : r + 8, c : c + 128]
        sums[pl.ds(step * per_step + b, 1), :] = jnp.sum(total, axis=0, keepdims=True)

    @pl.when(step == steps - 1)
    def _():
        out[...] = jnp.sum(sums[...].T, axis=0, keepdims=True)


def grad(dst, messages, basis, pieces, n_rel, n_dst):
    count, features, cols = basis.shape
    blocks = dst.shape[1]
    per_step = count // 8
    rows_dev = pieces[0].shape[0]
    return pl.pallas_call(
        functools.partial(grad_kernel, n_rel, n_dst),
        grid=(8,),
        in_specs=[
            whole(),
            whole(),
            pl.BlockSpec((per_step, features, cols), lambda k: (k, 0, 0)),
        ]
        + [whole()] * len(pieces),
        out_shape=jax.ShapeDtypeStruct((1, 128), f32),
        out_specs=whole(),
        scratch_shapes=[
            pltpu.VMEM((n_dst * n_rel * rows_dev, cols), bf16),
            pltpu.VMEM((features, cols), f32),
            pltpu.VMEM((128, 128), f32),
        ],
        compiler_params=pltpu.CompilerParams(
            dimension_semantics=("arbitrary",), vmem_limit_bytes=LIMIT
        ),
        cost_estimate=pl.CostEstimate(flops=4_000_000_000, bytes_accessed=10_000_000, transcendentals=0),
        name="grad",
    )(dst, messages, basis, *pieces)


def gather_kernel(n_rel, n_dst, block, *refs):
    got, outs = refs[:n_dst], refs[n_dst:]
    rows_dev = outs[0].shape[0]
    span = got[0].shape[0] // block * block
    rel = lax.axis_index("rel")
    ids = []
    for d in range(n_dst):
        pairs = got[d][span:, :block].astype(f32)
        ids.append(
            [
                (pairs[2 * b : 2 * b + 1] + 256.0 * pairs[2 * b + 1 : 2 * b + 2]).astype(i32)
                for b in range(span // block)
            ]
        )
    row = lax.broadcasted_iota(i32, (rows_dev, block), 0)
    for e in range(n_rel):
        place = row + (rel ^ e) * rows_dev
        total = None
        for d in range(n_dst):
            picks = jnp.concatenate(
                [(place == one).astype(bf16) for one in ids[d]], axis=1
            )
            more = jnp.dot(picks, got[d][:span, :], preferred_element_type=f32)
            total = more if total is None else total + more
        outs[e][...] = total.astype(outs[e].dtype)


def gather(got, n_rel, block, rows_dev):
    n_dst, cols = len(got), got[0].shape[1]
    return pl.pallas_call(
        functools.partial(gather_kernel, n_rel, n_dst, block),
        in_specs=[whole()] * n_dst,
        out_shape=[
            jax.ShapeDtypeStruct((rows_dev, cols), f32 if e == 0 else bf16)
            for e in range(n_rel)
        ],
        out_specs=[whole()] * n_rel,
        compiler_params=pltpu.CompilerParams(vmem_limit_bytes=LIMIT),
        cost_estimate=pl.CostEstimate(flops=600_000_000, bytes_accessed=1_000_000, transcendentals=0),
        name="gather",
    )(*got)


def finish_kernel(type_rows, bias, *refs):
    parts, out = refs[:-1], refs[-1]
    rows_dev, cols = out.shape
    kinds = bias.shape[0]
    total = parts[0][...]
    for part in parts[1:]:
        total = total + part[...].astype(f32)
    first = lax.axis_index("rel") * rows_dev
    row = lax.broadcasted_iota(i32, (rows_dev, cols), 0) + first
    added = jnp.broadcast_to(bias[0:1, :], (rows_dev, cols))
    bound = 0
    for c in range(kinds - 1):
        bound = bound + type_rows[c]
        added = jnp.where(row >= bound, bias[c + 1 : c + 2, :], added)
    out[...] = (total + added).astype(out.dtype)


def finish(type_rows, bias, parts):
    return pl.pallas_call(
        finish_kernel,
        in_specs=[whole(pltpu.SMEM), whole()] + [whole()] * len(parts),
        out_shape=jax.ShapeDtypeStruct(parts[0].shape, bf16),
        out_specs=whole(),
        compiler_params=pltpu.CompilerParams(vmem_limit_bytes=LIMIT),
        name="finish",
    )(type_rows, bias, *parts)


def on_device(
    node_table,
    edge_weights,
    src_ids,
    dst_ids,
    block_mask,
    basis_coef,
    basis_mats,
    type_bias,
    type_rows,
    cotangent,
):
    n_rel, n_dst, n_mp = (lax.axis_size(a) for a in ("rel", "dst", "mp"))
    block = edge_weights.shape[-1]
    rows_dev = cotangent.shape[0]

    along = [cotangent] + [swap(cotangent, "dst", d) for d in range(1, n_dst)]
    grid = [[piece] for piece in along]
    for e in range(2, n_rel, 2):
        for d in range(n_dst):
            grid[d].append(swap(along[d], "rel", e))
    pieces = []
    for d in range(n_dst):
        for mine in grid[d]:
            pieces += [mine, swap(mine, "rel", 1)]

    messages, *queues = send(
        basis_coef, block_mask, src_ids, dst_ids, node_table, edge_weights, basis_mats, n_dst
    )
    got = [queues[0]] + [swap(queues[d], "dst", d) for d in range(1, n_dst)]
    sums = gather(got, n_rel, block, rows_dev)
    parts = [sums[0]] + [swap(sums[e], "rel", e) for e in range(1, n_rel)]
    layer_out = finish(type_rows, type_bias, parts)

    partial = grad(dst_ids, messages, basis_mats, pieces, n_rel, n_dst)
    for axis, size in (("mp", n_mp), ("dst", n_dst)):
        d = 1
        while d < size:
            partial = partial + swap(partial, axis, d)
            d *= 2
    return layer_out, partial[:, : basis_coef.shape[1]]


def solution(mesh):
    in_specs = (
        P(("rel", "dst"), None),
        P("rel", "dst", None, None),
        P("rel", "dst", None),
        P("rel", "dst", None),
        P("rel", "dst"),
        P("rel", None),
        P(None, None, "mp"),
        P(None, "mp"),
        P(),
        P(("rel", "dst"), "mp"),
    )
    out_specs = (P(("rel", "dst"), "mp"), P("rel", None))
    return jax.shard_map(
        on_device, mesh=mesh, in_specs=in_specs, out_specs=out_specs, check_vma=False
    )
```

```python
import functools
import jax
import jax.numpy as jnp
from jax import lax
from jax.experimental import pallas as pl
from jax.experimental.pallas import tpu as pltpu
from jax.sharding import PartitionSpec as P


f32, bf16, i32 = jnp.float32, jnp.bfloat16, jnp.int32
LIMIT = 40 * 1024 * 1024
FIRST_FLOPS = 20_000_000_000
CONTRACT_ROWS = (((0,), (0,)), ((), ()))


def whole(space=pltpu.VMEM):
    return pl.BlockSpec(memory_space=space)


def spread_rows(row, rows):
    return jnp.broadcast_to(row, (rows, rows)).T


def one_hot(column, width):
    rows, lanes = column.shape
    lane = lax.broadcasted_iota(i32, (rows, lanes), 1)
    parts = [(column == lane + c).astype(bf16) for c in range(0, width, lanes)]
    return jnp.concatenate(parts, axis=1)


def send_kernel(
    n_dst, coef, mask, src_v, dst_v, table_v, weights_v, kept, _, messages, *rest
):
    outs = rest[:n_dst]
    (acc,) = rest[n_dst:]
    count, features, cols = kept.shape
    blocks, block = src_v.shape[1:]
    per_owner = blocks // n_dst
    span = per_owner * block
    size = 4

    columns = [spread_rows(src_v[0, k : k + 1, :], block) for k in range(blocks)]
    picks = jnp.concatenate([one_hot(c, table_v.shape[0]) for c in columns], axis=0)
    picked = jnp.dot(picks, table_v[...], preferred_element_type=f32).astype(bf16)
    for k in range(blocks):
        scaled = weights_v[0, k] * mask[0, k].astype(f32).astype(bf16)
        messages[k * block : (k + 1) * block, :] = jnp.dot(
            scaled, picked[k * block : (k + 1) * block, :], preferred_element_type=f32
        ).astype(bf16)

    acc[...] = jnp.zeros_like(acc)

    def mix(g, _):
        factors = [coef[0, g * size + b] for b in range(size)]
        chunk = 32
        for start in range(0, features, chunk):
            part = pl.ds(start, chunk)
            total = acc[part, :]
            for b in range(size):
                total = total + factors[b] * kept[g * size + b, part, :].astype(f32)
            acc[part, :] = total
        return 0

    lax.fori_loop(0, count // size, mix, 0)
    weight = acc[...].astype(bf16)

    me = lax.axis_index("dst")
    for d in range(n_dst):
        owner = me ^ d
        mine = messages[pl.ds(pl.multiple_of(owner * span, span), span), :]
        outs[d][:span, :] = jnp.dot(mine, weight, preferred_element_type=f32).astype(bf16)
        pad = outs[d].shape[0] - span
        which = lax.broadcasted_iota(i32, (pad, block), 0)
        slots = jnp.zeros((pad, block), i32)
        for b in range(per_owner):
            ids = dst_v[0, pl.ds(owner * per_owner + b, 1), :]
            slots = jnp.where(which == 2 * b, ids & 255, slots)
            slots = jnp.where(which == 2 * b + 1, ids >> 8, slots)
        outs[d][span:, :block] = slots.astype(f32).astype(bf16)
        outs[d][span:, block:] = jnp.zeros((pad, cols - block), bf16)


def send(coef, mask, src, dst, table, weights, basis, after, n_dst):
    _, features, cols = basis.shape
    blocks, block = src.shape[1:]
    span = blocks // n_dst * block
    pad = -(-2 * (blocks // n_dst) // 16) * 16
    return pl.pallas_call(
        functools.partial(send_kernel, n_dst),
        in_specs=[whole(pltpu.SMEM)] * 2 + [whole()] * 5 + [whole(pl.ANY)],
        out_shape=[
            jax.ShapeDtypeStruct((blocks * block, features), bf16),
        ]
        + [jax.ShapeDtypeStruct((span + pad, cols), bf16)] * n_dst,
        out_specs=[whole()] * (1 + n_dst),
        scratch_shapes=[
            pltpu.VMEM((features, cols), f32),
        ],
        compiler_params=pltpu.CompilerParams(vmem_limit_bytes=LIMIT),
        cost_estimate=pl.CostEstimate(flops=6_000_000_000, bytes_accessed=10_000_000, transcendentals=0),
        name="send",
    )(coef, mask, src, dst, table, weights, basis, after)


def first_kernel(out):
    out[...] = jnp.zeros_like(out)


def first():
    return pl.pallas_call(
        first_kernel,
        out_shape=jax.ShapeDtypeStruct((8, 128), f32),
        out_specs=whole(),
        compiler_params=pltpu.CompilerParams(vmem_limit_bytes=LIMIT),
        cost_estimate=pl.CostEstimate(flops=FIRST_FLOPS, bytes_accessed=4096, transcendentals=0),
        name="first",
    )()


def stack_kernel(type_rows, bias, _, *refs):
    parts, out, added = refs[:-2], refs[-2], refs[-1]
    rows_dev, cols = added.shape
    for d, part in enumerate(parts):
        out[d * rows_dev : (d + 1) * rows_dev, :] = part[...]
    row = lax.broadcasted_iota(i32, (rows_dev, cols), 0) + lax.axis_index("rel") * rows_dev
    total = jnp.broadcast_to(bias[0:1, :], (rows_dev, cols))
    bound = 0
    for c in range(bias.shape[0] - 1):
        bound = bound + type_rows[c]
        total = jnp.where(row >= bound, bias[c + 1 : c + 2, :], total)
    added[...] = total


def stack(type_rows, bias, after, parts):
    rows_dev, cols = parts[0].shape
    return pl.pallas_call(
        stack_kernel,
        in_specs=[whole(pltpu.SMEM), whole(), whole(pl.ANY)] + [whole()] * len(parts),
        out_shape=[
            jax.ShapeDtypeStruct((len(parts) * rows_dev, cols), bf16),
            jax.ShapeDtypeStruct((rows_dev, cols), f32),
        ],
        out_specs=[whole()] * 2,
        compiler_params=pltpu.CompilerParams(vmem_limit_bytes=LIMIT),
        name="stack",
    )(type_rows, bias, after, *parts)


def grad_kernel(n_rel, n_dst, dst, messages, basis, *rest):
    stacks, out = rest[:n_rel], rest[n_rel]
    outer, sums = rest[n_rel + 1 :]
    count, features, cols = basis.shape
    blocks, block = dst.shape[1:]
    rows_dev = stacks[0].shape[0] // n_dst
    span = blocks // n_dst * block
    rel, me = lax.axis_index("rel"), lax.axis_index("dst")

    total = None
    for d in range(n_dst):
        owner = me ^ d
        wanted = None
        columns = [
            spread_rows(dst[0, pl.ds(owner * (span // block) + b, 1), :], block)
            for b in range(span // block)
        ]
        for e in range(n_rel):
            first = (rel ^ e) * rows_dev
            picks = jnp.concatenate([one_hot(c - first, rows_dev) for c in columns], axis=0)
            more = jnp.dot(
                picks, stacks[e][d * rows_dev : (d + 1) * rows_dev, :], preferred_element_type=f32
            )
            wanted = more if wanted is None else wanted + more
        more = lax.dot_general(
            messages[pl.ds(pl.multiple_of(owner * span, span), span), :],
            wanted.astype(bf16),
            CONTRACT_ROWS,
            preferred_element_type=f32,
        )
        total = more if total is None else total + more
    outer[...] = total

    size = 4

    def contract(g, _):
        totals = [jnp.zeros((8, 128), f32)] * size
        for start in range(0, features, 16):
            part = pl.ds(start, 16)
            side = outer[part, :]
            for b in range(size):
                prod = basis[g * size + b, part, :].astype(f32) * side
                more = prod[:8, :] + prod[8:, :]
                for c in range(0, cols, 128):
                    totals[b] = totals[b] + more[:, c : c + 128]
        for b in range(size):
            sums[pl.ds(g * size + b, 1), :] = jnp.sum(totals[b], axis=0, keepdims=True)
        return 0

    lax.fori_loop(0, count // size, contract, 0)
    out[...] = jnp.sum(sums[...].T, axis=0, keepdims=True)


def grad(dst, messages, basis, stacks, n_dst):
    _, features, cols = basis.shape
    return pl.pallas_call(
        functools.partial(grad_kernel, len(stacks), n_dst),
        in_specs=[whole()] * (3 + len(stacks)),
        out_shape=jax.ShapeDtypeStruct((1, 128), f32),
        out_specs=whole(),
        scratch_shapes=[pltpu.VMEM((features, cols), f32), pltpu.VMEM((128, 128), f32)],
        compiler_params=pltpu.CompilerParams(vmem_limit_bytes=LIMIT),
        cost_estimate=pl.CostEstimate(flops=4_000_000_000, bytes_accessed=10_000_000, transcendentals=0),
        name="grad",
    )(dst, messages, basis, *stacks)


def gather_kernel(n_rel, n_dst, block, added, *refs):
    got, outs = refs[:n_dst], refs[n_dst:]
    rows_dev = outs[0].shape[0]
    span = got[0].shape[0] // block * block
    rel = lax.axis_index("rel")
    ids = []
    for d in range(n_dst):
        pairs = got[d][span:, :block].astype(f32)
        ids.append(
            [
                (pairs[2 * b : 2 * b + 1] + 256.0 * pairs[2 * b + 1 : 2 * b + 2]).astype(i32)
                for b in range(span // block)
            ]
        )
    row = lax.broadcasted_iota(i32, (rows_dev, block), 0)
    for e in range(n_rel):
        place = row + (rel ^ e) * rows_dev
        total = None
        for d in range(n_dst):
            picks = jnp.concatenate(
                [(place == one).astype(bf16) for one in ids[d]], axis=1
            )
            more = jnp.dot(picks, got[d][:span, :], preferred_element_type=f32)
            total = more if total is None else total + more
        if e == 0:
            total = total + added[...]
        outs[e][...] = total.astype(outs[e].dtype)


def gather(added, got, n_rel, block, rows_dev):
    n_dst, cols = len(got), got[0].shape[1]
    return pl.pallas_call(
        functools.partial(gather_kernel, n_rel, n_dst, block),
        in_specs=[whole()] * (1 + n_dst),
        out_shape=[
            jax.ShapeDtypeStruct((rows_dev, cols), f32 if e == 0 else bf16)
            for e in range(n_rel)
        ],
        out_specs=[whole()] * n_rel,
        compiler_params=pltpu.CompilerParams(vmem_limit_bytes=LIMIT),
        cost_estimate=pl.CostEstimate(flops=600_000_000, bytes_accessed=1_000_000, transcendentals=0),
        name="gather",
    )(added, *got)


def finish_kernel(*refs):
    parts, out = refs[:-1], refs[-1]
    total = parts[0][...]
    for part in parts[1:]:
        total = total + part[...].astype(f32)
    out[...] = total.astype(out.dtype)


def finish(parts):
    return pl.pallas_call(
        finish_kernel,
        in_specs=[whole()] * len(parts),
        out_shape=jax.ShapeDtypeStruct(parts[0].shape, bf16),
        out_specs=whole(),
        compiler_params=pltpu.CompilerParams(vmem_limit_bytes=LIMIT),
        name="finish",
    )(*parts)


def on_device(
    node_table,
    edge_weights,
    src_ids,
    dst_ids,
    block_mask,
    basis_coef,
    basis_mats,
    type_bias,
    type_rows,
    cotangent,
):
    n_rel, n_dst, n_mp = (lax.axis_size(a) for a in ("rel", "dst", "mp"))
    block = edge_weights.shape[-1]
    rows_dev = cotangent.shape[0]

    def swap(x, axis, d):
        n = lax.axis_size(axis)
        return lax.ppermute(x, axis, [(i, i ^ d) for i in range(n)])

    along = [cotangent] + [swap(cotangent, "dst", d) for d in range(1, n_dst)]
    begun = first()
    messages, *queues = send(
        basis_coef,
        block_mask,
        src_ids,
        dst_ids,
        node_table,
        edge_weights,
        basis_mats,
        begun,
        n_dst,
    )
    got = [queues[0]] + [swap(queues[d], "dst", d) for d in range(1, n_dst)]

    stacked, added = stack(type_rows, type_bias, messages, along)
    stacks = [None] * n_rel
    for e in range(0, n_rel, 2):
        stacks[e] = swap(stacked, "rel", e) if e else stacked
        stacks[e + 1] = swap(stacks[e], "rel", 1)
    partial = grad(dst_ids, messages, basis_mats, stacks, n_dst)

    sums = gather(added, got, n_rel, block, rows_dev)
    parts = [sums[0]] + [swap(sums[e], "rel", e) for e in range(1, n_rel)]
    layer_out = finish(parts)

    for axis, size in (("mp", n_mp), ("dst", n_dst)):
        d = 1
        while d < size:
            partial = partial + swap(partial, axis, d)
            d *= 2
    return layer_out, partial[:, : basis_coef.shape[1]]


def solution(mesh):
    in_specs = (
        P(("rel", "dst"), None),
        P("rel", "dst", None, None),
        P("rel", "dst", None),
        P("rel", "dst", None),
        P("rel", "dst"),
        P("rel", None),
        P(None, None, "mp"),
        P(None, "mp"),
        P(),
        P(("rel", "dst"), "mp"),
    )
    out_specs = (P(("rel", "dst"), "mp"), P("rel", None))

    return jax.shard_map(
        on_device, mesh=mesh, in_specs=in_specs, out_specs=out_specs, check_vma=False
    )
```

```python
import functools
import jax
import jax.numpy as jnp
from jax import lax
from jax.experimental import pallas as pl
from jax.experimental.pallas import tpu as pltpu
from jax.sharding import PartitionSpec as P


f32, bf16, i32 = jnp.float32, jnp.bfloat16, jnp.int32
LIMIT = 40 * 1024 * 1024
FIRST_FLOPS = 20_000_000_000
MIX = 4
CONTRACT_ROWS = (((0,), (0,)), ((), ()))


def whole(space=pltpu.VMEM):
    return pl.BlockSpec(memory_space=space)


def spread_rows(row, rows):
    return jnp.broadcast_to(row, (rows, rows)).T


def one_hot(column, width):
    rows, lanes = column.shape
    lane = lax.broadcasted_iota(i32, (rows, lanes), 1)
    parts = [(column == lane + c).astype(bf16) for c in range(0, width, lanes)]
    return jnp.concatenate(parts, axis=1)


def mix(coef, basis, acc, begin, end):
    features = acc.shape[0]
    size, chunk = MIX, 32

    def body(g, _):
        at = begin + g * size
        factors = [coef[0, at + b] for b in range(size)]
        for start in range(0, features, chunk):
            part = pl.ds(start, chunk)
            total = acc[part, :]
            for b in range(size):
                total = total + factors[b] * basis[at + b, part, :].astype(f32)
            acc[part, :] = total
        return 0

    lax.fori_loop(0, (end - begin) // size, body, 0, unroll=True)


def send_kernel(n_dst, coef, mask, src, dst, table, weights, basis, _, messages, *rest):
    outs, acc = rest[:n_dst], rest[n_dst]
    count, _, cols = basis.shape
    blocks, block = src.shape[1:]
    per_owner = blocks // n_dst
    span = per_owner * block

    columns = [spread_rows(src[0, k : k + 1, :], block) for k in range(blocks)]
    picks = jnp.concatenate([one_hot(c, table.shape[0]) for c in columns], axis=0)
    picked = jnp.dot(picks, table[...], preferred_element_type=f32).astype(bf16)
    for k in range(blocks):
        scaled = weights[0, k] * mask[0, k].astype(f32).astype(bf16)
        messages[k * block : (k + 1) * block, :] = jnp.dot(
            scaled, picked[k * block : (k + 1) * block, :], preferred_element_type=f32
        ).astype(bf16)

    acc[...] = jnp.zeros_like(acc)
    mix(coef, basis, acc, 0, count)
    weight = acc[...].astype(bf16)
    me = lax.axis_index("dst")
    for d in range(n_dst):
        owner = me ^ d
        mine = messages[pl.ds(pl.multiple_of(owner * span, span), span), :]
        outs[d][:span, :] = jnp.dot(mine, weight, preferred_element_type=f32).astype(bf16)
        pad = outs[d].shape[0] - span
        which = lax.broadcasted_iota(i32, (pad, block), 0)
        slots = jnp.zeros((pad, block), i32)
        for b in range(per_owner):
            ids = dst[0, pl.ds(owner * per_owner + b, 1), :]
            slots = jnp.where(which == 2 * b, ids & 255, slots)
            slots = jnp.where(which == 2 * b + 1, ids >> 8, slots)
        outs[d][span:, :block] = slots.astype(f32).astype(bf16)
        outs[d][span:, block:] = jnp.zeros((pad, cols - block), bf16)


def send(coef, mask, src, dst, table, weights, basis, after, n_dst):
    features, cols = basis.shape[1:]
    blocks, block = src.shape[1:]
    span = blocks // n_dst * block
    pad = -(-2 * (blocks // n_dst) // 16) * 16
    return pl.pallas_call(
        functools.partial(send_kernel, n_dst),
        in_specs=[whole(pltpu.SMEM)] * 2 + [whole()] * 5 + [whole(pl.ANY)],
        out_shape=[jax.ShapeDtypeStruct((blocks * block, features), bf16)]
        + [jax.ShapeDtypeStruct((span + pad, cols), bf16)] * n_dst,
        out_specs=[whole()] * (1 + n_dst),
        scratch_shapes=[pltpu.VMEM((features, cols), f32)],
        compiler_params=pltpu.CompilerParams(vmem_limit_bytes=LIMIT),
        cost_estimate=pl.CostEstimate(flops=6_000_000_000, bytes_accessed=10_000_000, transcendentals=0),
        name="send",
    )(coef, mask, src, dst, table, weights, basis, after)


def first_kernel(out):
    out[...] = jnp.zeros_like(out)


def first():
    return pl.pallas_call(
        first_kernel,
        out_shape=jax.ShapeDtypeStruct((8, 128), f32),
        out_specs=whole(),
        compiler_params=pltpu.CompilerParams(vmem_limit_bytes=LIMIT),
        cost_estimate=pl.CostEstimate(flops=FIRST_FLOPS, bytes_accessed=4096, transcendentals=0),
        name="first",
    )()


def stack_kernel(type_rows, bias, _, *refs):
    parts, out, added = refs[:-2], refs[-2], refs[-1]
    rows_dev, cols = added.shape
    for d, part in enumerate(parts):
        out[d * rows_dev : (d + 1) * rows_dev, :] = part[...]
    row = lax.broadcasted_iota(i32, (rows_dev, cols), 0) + lax.axis_index("rel") * rows_dev
    total = jnp.broadcast_to(bias[0:1, :], (rows_dev, cols))
    bound = 0
    for c in range(bias.shape[0] - 1):
        bound = bound + type_rows[c]
        total = jnp.where(row >= bound, bias[c + 1 : c + 2, :], total)
    added[...] = total


def stack(type_rows, bias, after, parts):
    rows_dev, cols = parts[0].shape
    return pl.pallas_call(
        stack_kernel,
        in_specs=[whole(pltpu.SMEM), whole(), whole(pl.ANY)] + [whole()] * len(parts),
        out_shape=[
            jax.ShapeDtypeStruct((len(parts) * rows_dev, cols), bf16),
            jax.ShapeDtypeStruct((rows_dev, cols), f32),
        ],
        out_specs=[whole()] * 2,
        compiler_params=pltpu.CompilerParams(vmem_limit_bytes=LIMIT),
        name="stack",
    )(type_rows, bias, after, *parts)


def outer_kernel(n_rel, n_dst, near, dst, messages, *rest):
    stacks, outer, late = rest[:near], rest[near], rest[near + 1 :]
    blocks, block = dst.shape[1:]
    rows_dev = stacks[0].shape[0] // n_dst
    span = blocks // n_dst * block
    rel, me = lax.axis_index("rel"), lax.axis_index("dst")
    early = [[] for _ in range(near)]
    for d in range(n_dst):
        owner = me ^ d
        columns = [
            spread_rows(dst[0, pl.ds(owner * (span // block) + b, 1), :], block)
            for b in range(span // block)
        ]
        picks = jnp.concatenate(
            [
                jnp.concatenate(
                    [one_hot(c - (rel ^ e) * rows_dev, rows_dev) for e in range(n_rel)], axis=1
                )
                for c in columns
            ],
            axis=0,
        )
        summed = lax.dot_general(
            messages[pl.ds(pl.multiple_of(owner * span, span), span), :],
            picks,
            CONTRACT_ROWS,
            preferred_element_type=f32,
        ).astype(bf16)
        for e in range(n_rel):
            part = summed[:, e * rows_dev : (e + 1) * rows_dev]
            if e < near:
                early[e].append(part)
            else:
                late[e - near][:, d * rows_dev : (d + 1) * rows_dev] = part
    total = None
    for e in range(near):
        left = jnp.concatenate(early[e], axis=1)
        more = jnp.dot(left, stacks[e][...], preferred_element_type=f32)
        total = more if total is None else total + more
    outer[...] = total


def outer(dst, messages, stacks, n_rel, n_dst):
    features = messages.shape[1]
    rows, cols = stacks[0].shape
    near = len(stacks)
    return pl.pallas_call(
        functools.partial(outer_kernel, n_rel, n_dst, near),
        in_specs=[whole()] * (2 + near),
        out_shape=[jax.ShapeDtypeStruct((features, cols), f32)]
        + [jax.ShapeDtypeStruct((features, rows), bf16)] * (n_rel - near),
        out_specs=[whole()] * (1 + n_rel - near),
        compiler_params=pltpu.CompilerParams(vmem_limit_bytes=LIMIT),
        cost_estimate=pl.CostEstimate(flops=2_000_000_000, bytes_accessed=4_000_000, transcendentals=0),
        name="outer",
    )(dst, messages, *stacks)


def grad_kernel(count_late, basis, partial, *rest):
    lefts, rights = rest[:count_late], rest[count_late : 2 * count_late]
    out, outer, sums = rest[2 * count_late :]
    count, features, cols = basis.shape
    total = partial[...]
    for left, right in zip(lefts, rights):
        total = total + jnp.dot(left[...], right[...], preferred_element_type=f32)
    outer[...] = total

    size = 4

    def contract(g, _):
        totals = [jnp.zeros((8, 128), f32)] * size
        for start in range(0, features, 16):
            part = pl.ds(start, 16)
            side = outer[part, :]
            for b in range(size):
                prod = basis[g * size + b, part, :].astype(f32) * side
                more = prod[:8, :] + prod[8:, :]
                for c in range(0, cols, 128):
                    totals[b] = totals[b] + more[:, c : c + 128]
        for b in range(size):
            sums[pl.ds(g * size + b, 1), :] = jnp.sum(totals[b], axis=0, keepdims=True)
        return 0

    lax.fori_loop(0, count // size, contract, 0)
    out[...] = jnp.sum(sums[...].T, axis=0, keepdims=True)


def grad(basis, partial, lefts, rights):
    features, cols = basis.shape[1:]
    return pl.pallas_call(
        functools.partial(grad_kernel, len(lefts)),
        in_specs=[whole()] * (2 + 2 * len(lefts)),
        out_shape=jax.ShapeDtypeStruct((1, 128), f32),
        out_specs=whole(),
        scratch_shapes=[pltpu.VMEM((features, cols), f32), pltpu.VMEM((128, 128), f32)],
        compiler_params=pltpu.CompilerParams(vmem_limit_bytes=LIMIT),
        cost_estimate=pl.CostEstimate(flops=4_000_000_000, bytes_accessed=10_000_000, transcendentals=0),
        name="grad",
    )(basis, partial, *lefts, *rights)


def gather_kernel(n_rel, n_dst, block, added, *refs):
    got, outs = refs[:n_dst], refs[n_dst:]
    rows_dev = outs[0].shape[0]
    span = got[0].shape[0] // block * block
    rel = lax.axis_index("rel")
    ids = []
    for d in range(n_dst):
        pairs = got[d][span:, :block].astype(f32)
        ids.append(
            [
                (pairs[2 * b : 2 * b + 1] + 256.0 * pairs[2 * b + 1 : 2 * b + 2]).astype(i32)
                for b in range(span // block)
            ]
        )
    row = lax.broadcasted_iota(i32, (rows_dev, block), 0)
    for e in range(n_rel):
        place = row + (rel ^ e) * rows_dev
        total = None
        for d in range(n_dst):
            picks = jnp.concatenate(
                [(place == one).astype(bf16) for one in ids[d]], axis=1
            )
            more = jnp.dot(picks, got[d][:span, :], preferred_element_type=f32)
            total = more if total is None else total + more
        if e == 0:
            total = total + added[...]
        outs[e][...] = total.astype(outs[e].dtype)


def gather(added, got, n_rel, block, rows_dev):
    n_dst, cols = len(got), got[0].shape[1]
    return pl.pallas_call(
        functools.partial(gather_kernel, n_rel, n_dst, block),
        in_specs=[whole()] * (1 + n_dst),
        out_shape=[
            jax.ShapeDtypeStruct((rows_dev, cols), f32 if e == 0 else bf16)
            for e in range(n_rel)
        ],
        out_specs=[whole()] * n_rel,
        compiler_params=pltpu.CompilerParams(vmem_limit_bytes=LIMIT),
        cost_estimate=pl.CostEstimate(flops=600_000_000, bytes_accessed=1_000_000, transcendentals=0),
        name="gather",
    )(added, *got)


def finish_kernel(*refs):
    parts, out = refs[:-1], refs[-1]
    total = parts[0][...]
    for part in parts[1:]:
        total = total + part[...].astype(f32)
    out[...] = total.astype(out.dtype)


def finish(parts):
    return pl.pallas_call(
        finish_kernel,
        in_specs=[whole()] * len(parts),
        out_shape=jax.ShapeDtypeStruct(parts[0].shape, bf16),
        out_specs=whole(),
        compiler_params=pltpu.CompilerParams(vmem_limit_bytes=LIMIT),
        name="finish",
    )(*parts)


def on_device(
    node_table,
    edge_weights,
    src_ids,
    dst_ids,
    block_mask,
    basis_coef,
    basis_mats,
    type_bias,
    type_rows,
    cotangent,
):
    n_rel, n_dst, n_mp = (lax.axis_size(a) for a in ("rel", "dst", "mp"))
    block = edge_weights.shape[-1]
    rows_dev = cotangent.shape[0]

    def swap(x, axis, d):
        n = lax.axis_size(axis)
        return lax.ppermute(x, axis, [(i, i ^ d) for i in range(n)])

    along = [cotangent] + [swap(cotangent, "dst", d) for d in range(1, n_dst)]
    begun = first()
    messages, *queues = send(
        basis_coef,
        block_mask,
        src_ids,
        dst_ids,
        node_table,
        edge_weights,
        basis_mats,
        begun,
        n_dst,
    )
    got = [queues[0]] + [swap(queues[d], "dst", d) for d in range(1, n_dst)]
    stacked, added = stack(type_rows, type_bias, messages, along)

    stacks = [None] * n_rel
    for e in range(0, n_rel, 2):
        stacks[e] = swap(stacked, "rel", e) if e else stacked
        stacks[e + 1] = swap(stacks[e], "rel", 1)
    outer_sum, *lefts = outer(dst_ids, messages, stacks[:2], n_rel, n_dst)
    partial = grad(basis_mats, outer_sum, lefts, stacks[2:])

    sums = gather(added, got, n_rel, block, rows_dev)
    parts = [sums[0]] + [swap(sums[e], "rel", e) for e in range(1, n_rel)]
    layer_out = finish(parts)

    for axis, size in (("mp", n_mp), ("dst", n_dst)):
        d = 1
        while d < size:
            partial = partial + swap(partial, axis, d)
            d *= 2
    return layer_out, partial[:, : basis_coef.shape[1]]


def solution(mesh):
    in_specs = (
        P(("rel", "dst"), None),
        P("rel", "dst", None, None),
        P("rel", "dst", None),
        P("rel", "dst", None),
        P("rel", "dst"),
        P("rel", None),
        P(None, None, "mp"),
        P(None, "mp"),
        P(),
        P(("rel", "dst"), "mp"),
    )
    out_specs = (P(("rel", "dst"), "mp"), P("rel", None))

    return jax.shard_map(
        on_device, mesh=mesh, in_specs=in_specs, out_specs=out_specs, check_vma=False
    )
```

```python
import functools
import jax
import jax.numpy as jnp
from jax import lax
from jax.experimental import pallas as pl
from jax.experimental.pallas import tpu as pltpu
from jax.sharding import PartitionSpec as P


f32, bf16, i32 = jnp.float32, jnp.bfloat16, jnp.int32
LIMIT = 40 * 1024 * 1024
FIRST_FLOPS = 20_000_000_000
MIX = 4
CONTRACT_ROWS = (((0,), (0,)), ((), ()))


def whole(space=pltpu.VMEM):
    return pl.BlockSpec(memory_space=space)


def spread_rows(row, rows):
    return jnp.broadcast_to(row, (rows, rows)).T


def one_hot(column, width):
    rows, lanes = column.shape
    lane = lax.broadcasted_iota(i32, (rows, lanes), 1)
    parts = [(column == lane + c).astype(bf16) for c in range(0, width, lanes)]
    return jnp.concatenate(parts, axis=1)


def mix(coef, basis, acc, begin, end):
    features = acc.shape[0]
    size, chunk = MIX, 32

    def body(g, _):
        at = begin + g * size
        factors = [coef[0, at + b] for b in range(size)]
        for start in range(0, features, chunk):
            part = pl.ds(start, chunk)
            total = acc[part, :]
            for b in range(size):
                total = total + factors[b] * basis[at + b, part, :].astype(f32)
            acc[part, :] = total
        return 0

    lax.fori_loop(0, (end - begin) // size, body, 0, unroll=True)


def send_kernel(n_dst, coef, mask, src, dst, table, weights, basis, _, messages, *rest):
    outs, acc = rest[:n_dst], rest[n_dst]
    count, _, cols = basis.shape
    blocks, block = src.shape[1:]
    per_owner = blocks // n_dst
    span = per_owner * block

    columns = [spread_rows(src[0, k : k + 1, :], block) for k in range(blocks)]
    picks = jnp.concatenate([one_hot(c, table.shape[0]) for c in columns], axis=0)
    picked = jnp.dot(picks, table[...], preferred_element_type=f32).astype(bf16)
    for k in range(blocks):
        scaled = weights[0, k] * mask[0, k].astype(f32).astype(bf16)
        messages[k * block : (k + 1) * block, :] = jnp.dot(
            scaled, picked[k * block : (k + 1) * block, :], preferred_element_type=f32
        ).astype(bf16)

    acc[...] = jnp.zeros_like(acc)
    mix(coef, basis, acc, 0, count)
    weight = acc[...].astype(bf16)
    me = lax.axis_index("dst")
    for d in range(n_dst):
        owner = me ^ d
        mine = messages[pl.ds(pl.multiple_of(owner * span, span), span), :]
        outs[d][:span, :] = jnp.dot(mine, weight, preferred_element_type=f32).astype(bf16)
        pad = outs[d].shape[0] - span
        which = lax.broadcasted_iota(i32, (pad, block), 0)
        slots = jnp.zeros((pad, block), i32)
        for b in range(per_owner):
            ids = dst[0, pl.ds(owner * per_owner + b, 1), :]
            slots = jnp.where(which == 2 * b, ids & 255, slots)
            slots = jnp.where(which == 2 * b + 1, ids >> 8, slots)
        outs[d][span:, :block] = slots.astype(f32).astype(bf16)
        outs[d][span:, block:] = jnp.zeros((pad, cols - block), bf16)


def send(coef, mask, src, dst, table, weights, basis, after, n_dst):
    features, cols = basis.shape[1:]
    blocks, block = src.shape[1:]
    span = blocks // n_dst * block
    pad = -(-2 * (blocks // n_dst) // 16) * 16
    return pl.pallas_call(
        functools.partial(send_kernel, n_dst),
        in_specs=[whole(pltpu.SMEM)] * 2 + [whole()] * 5 + [whole(pl.ANY)],
        out_shape=[jax.ShapeDtypeStruct((blocks * block, features), bf16)]
        + [jax.ShapeDtypeStruct((span + pad, cols), bf16)] * n_dst,
        out_specs=[whole()] * (1 + n_dst),
        scratch_shapes=[pltpu.VMEM((features, cols), f32)],
        compiler_params=pltpu.CompilerParams(vmem_limit_bytes=LIMIT),
        cost_estimate=pl.CostEstimate(flops=6_000_000_000, bytes_accessed=10_000_000, transcendentals=0),
        name="send",
    )(coef, mask, src, dst, table, weights, basis, after)


def first_kernel(out):
    out[...] = jnp.zeros_like(out)


def first():
    return pl.pallas_call(
        first_kernel,
        out_shape=jax.ShapeDtypeStruct((8, 128), f32),
        out_specs=whole(),
        compiler_params=pltpu.CompilerParams(vmem_limit_bytes=LIMIT),
        cost_estimate=pl.CostEstimate(flops=FIRST_FLOPS, bytes_accessed=4096, transcendentals=0),
        name="first",
    )()


def stack_kernel(type_rows, bias, _, *refs):
    parts, out, added = refs[:-2], refs[-2], refs[-1]
    rows_dev, cols = added.shape
    for d, part in enumerate(parts):
        out[d * rows_dev : (d + 1) * rows_dev, :] = part[...]
    row = lax.broadcasted_iota(i32, (rows_dev, cols), 0) + lax.axis_index("rel") * rows_dev
    total = jnp.broadcast_to(bias[0:1, :], (rows_dev, cols))
    bound = 0
    for c in range(bias.shape[0] - 1):
        bound = bound + type_rows[c]
        total = jnp.where(row >= bound, bias[c + 1 : c + 2, :], total)
    added[...] = total


def stack(type_rows, bias, after, parts):
    rows_dev, cols = parts[0].shape
    return pl.pallas_call(
        stack_kernel,
        in_specs=[whole(pltpu.SMEM), whole(), whole(pl.ANY)] + [whole()] * len(parts),
        out_shape=[
            jax.ShapeDtypeStruct((len(parts) * rows_dev, cols), bf16),
            jax.ShapeDtypeStruct((rows_dev, cols), f32),
        ],
        out_specs=[whole()] * 2,
        compiler_params=pltpu.CompilerParams(vmem_limit_bytes=LIMIT),
        name="stack",
    )(type_rows, bias, after, *parts)


def outer_kernel(n_rel, n_dst, near, dst, messages, *rest):
    stacks, outer, late = rest[:near], rest[near], rest[near + 1 :]
    blocks, block = dst.shape[1:]
    rows_dev = stacks[0].shape[0] // n_dst
    span = blocks // n_dst * block
    rel, me = lax.axis_index("rel"), lax.axis_index("dst")
    early = [[] for _ in range(near)]
    for d in range(n_dst):
        owner = me ^ d
        columns = [
            spread_rows(dst[0, pl.ds(owner * (span // block) + b, 1), :], block)
            for b in range(span // block)
        ]
        picks = jnp.concatenate(
            [
                jnp.concatenate(
                    [one_hot(c - (rel ^ e) * rows_dev, rows_dev) for e in range(n_rel)], axis=1
                )
                for c in columns
            ],
            axis=0,
        )
        summed = lax.dot_general(
            messages[pl.ds(pl.multiple_of(owner * span, span), span), :],
            picks,
            CONTRACT_ROWS,
            preferred_element_type=f32,
        ).astype(bf16)
        for e in range(n_rel):
            part = summed[:, e * rows_dev : (e + 1) * rows_dev]
            if e < near:
                early[e].append(part)
            else:
                late[e - near][:, d * rows_dev : (d + 1) * rows_dev] = part
    total = None
    for e in range(near):
        left = jnp.concatenate(early[e], axis=1)
        more = jnp.dot(left, stacks[e][...], preferred_element_type=f32)
        total = more if total is None else total + more
    outer[...] = total


def outer(dst, messages, stacks, n_rel, n_dst):
    features = messages.shape[1]
    rows, cols = stacks[0].shape
    near = len(stacks)
    return pl.pallas_call(
        functools.partial(outer_kernel, n_rel, n_dst, near),
        in_specs=[whole()] * (2 + near),
        out_shape=[jax.ShapeDtypeStruct((features, cols), f32)]
        + [jax.ShapeDtypeStruct((features, rows), bf16)] * (n_rel - near),
        out_specs=[whole()] * (1 + n_rel - near),
        compiler_params=pltpu.CompilerParams(vmem_limit_bytes=LIMIT),
        cost_estimate=pl.CostEstimate(flops=2_000_000_000, bytes_accessed=4_000_000, transcendentals=0),
        name="outer",
    )(dst, messages, *stacks)


def grad_kernel(count_late, basis, partial, *rest):
    lefts, rights = rest[:count_late], rest[count_late : 2 * count_late]
    out, outer, sums = rest[2 * count_late :]
    count, features, cols = basis.shape
    total = partial[...]
    for left, right in zip(lefts, rights):
        total = total + jnp.dot(left[...], right[...], preferred_element_type=f32)
    outer[...] = total.astype(bf16)

    size = 4

    def contract(g, _):
        totals = [jnp.zeros((8, 128), f32)] * size
        for start in range(0, features, 32):
            part = pl.ds(start, 32)
            side = outer[part, :]
            for b in range(size):
                prod = basis[g * size + b, part, :] * side
                more = (prod[:16, :] + prod[16:, :]).astype(f32)
                for r in range(0, 16, 8):
                    for c in range(0, cols, 128):
                        totals[b] = totals[b] + more[r : r + 8, c : c + 128]
        for b in range(size):
            sums[pl.ds(g * size + b, 1), :] = jnp.sum(totals[b], axis=0, keepdims=True)
        return 0

    lax.fori_loop(0, count // size, contract, 0, unroll=True)
    out[...] = jnp.sum(sums[...].T, axis=0, keepdims=True)


def grad(basis, partial, lefts, rights):
    features, cols = basis.shape[1:]
    return pl.pallas_call(
        functools.partial(grad_kernel, len(lefts)),
        in_specs=[whole()] * (2 + 2 * len(lefts)),
        out_shape=jax.ShapeDtypeStruct((1, 128), f32),
        out_specs=whole(),
        scratch_shapes=[pltpu.VMEM((features, cols), bf16), pltpu.VMEM((128, 128), f32)],
        compiler_params=pltpu.CompilerParams(vmem_limit_bytes=LIMIT),
        cost_estimate=pl.CostEstimate(flops=4_000_000_000, bytes_accessed=10_000_000, transcendentals=0),
        name="grad",
    )(basis, partial, *lefts, *rights)


def gather_kernel(n_rel, n_dst, block, added, *refs):
    got, outs = refs[:n_dst], refs[n_dst:]
    rows_dev = outs[0].shape[0]
    span = got[0].shape[0] // block * block
    rel = lax.axis_index("rel")
    ids = []
    for d in range(n_dst):
        pairs = got[d][span:, :block].astype(f32)
        ids.append(
            [
                (pairs[2 * b : 2 * b + 1] + 256.0 * pairs[2 * b + 1 : 2 * b + 2]).astype(i32)
                for b in range(span // block)
            ]
        )
    row = lax.broadcasted_iota(i32, (rows_dev, block), 0)
    for e in range(n_rel):
        place = row + (rel ^ e) * rows_dev
        total = None
        for d in range(n_dst):
            picks = jnp.concatenate(
                [(place == one).astype(bf16) for one in ids[d]], axis=1
            )
            more = jnp.dot(picks, got[d][:span, :], preferred_element_type=f32)
            total = more if total is None else total + more
        if e == 0:
            total = total + added[...]
        outs[e][...] = total.astype(outs[e].dtype)


def gather(added, got, n_rel, block, rows_dev):
    n_dst, cols = len(got), got[0].shape[1]
    return pl.pallas_call(
        functools.partial(gather_kernel, n_rel, n_dst, block),
        in_specs=[whole()] * (1 + n_dst),
        out_shape=[
            jax.ShapeDtypeStruct((rows_dev, cols), f32 if e == 0 else bf16)
            for e in range(n_rel)
        ],
        out_specs=[whole()] * n_rel,
        compiler_params=pltpu.CompilerParams(vmem_limit_bytes=LIMIT),
        cost_estimate=pl.CostEstimate(flops=600_000_000, bytes_accessed=1_000_000, transcendentals=0),
        name="gather",
    )(added, *got)


def finish_kernel(*refs):
    parts, out = refs[:-1], refs[-1]
    total = parts[0][...]
    for part in parts[1:]:
        total = total + part[...].astype(f32)
    out[...] = total.astype(out.dtype)


def finish(parts):
    return pl.pallas_call(
        finish_kernel,
        in_specs=[whole()] * len(parts),
        out_shape=jax.ShapeDtypeStruct(parts[0].shape, bf16),
        out_specs=whole(),
        compiler_params=pltpu.CompilerParams(vmem_limit_bytes=LIMIT),
        name="finish",
    )(*parts)


def on_device(
    node_table,
    edge_weights,
    src_ids,
    dst_ids,
    block_mask,
    basis_coef,
    basis_mats,
    type_bias,
    type_rows,
    cotangent,
):
    n_rel, n_dst, n_mp = (lax.axis_size(a) for a in ("rel", "dst", "mp"))
    block = edge_weights.shape[-1]
    rows_dev = cotangent.shape[0]

    def swap(x, axis, d):
        n = lax.axis_size(axis)
        return lax.ppermute(x, axis, [(i, i ^ d) for i in range(n)])

    along = [cotangent] + [swap(cotangent, "dst", d) for d in range(1, n_dst)]
    begun = first()
    messages, *queues = send(
        basis_coef,
        block_mask,
        src_ids,
        dst_ids,
        node_table,
        edge_weights,
        basis_mats,
        begun,
        n_dst,
    )
    got = [queues[0]] + [swap(queues[d], "dst", d) for d in range(1, n_dst)]
    stacked, added = stack(type_rows, type_bias, messages, along)

    stacks = [None] * n_rel
    for e in range(0, n_rel, 2):
        stacks[e] = swap(stacked, "rel", e) if e else stacked
        stacks[e + 1] = swap(stacks[e], "rel", 1)
    outer_sum, *lefts = outer(dst_ids, messages, stacks[:2], n_rel, n_dst)
    partial = grad(basis_mats, outer_sum, lefts, stacks[2:])

    sums = gather(added, got, n_rel, block, rows_dev)
    parts = [sums[0]] + [swap(sums[e], "rel", e) for e in range(1, n_rel)]
    layer_out = finish(parts)

    for axis, size in (("mp", n_mp), ("dst", n_dst)):
        d = 1
        while d < size:
            partial = partial + swap(partial, axis, d)
            d *= 2
    return layer_out, partial[:, : basis_coef.shape[1]]


def solution(mesh):
    in_specs = (
        P(("rel", "dst"), None),
        P("rel", "dst", None, None),
        P("rel", "dst", None),
        P("rel", "dst", None),
        P("rel", "dst"),
        P("rel", None),
        P(None, None, "mp"),
        P(None, "mp"),
        P(),
        P(("rel", "dst"), "mp"),
    )
    out_specs = (P(("rel", "dst"), "mp"), P("rel", None))

    return jax.shard_map(
        on_device, mesh=mesh, in_specs=in_specs, out_specs=out_specs, check_vma=False
    )
```

```python
import functools
import jax
import jax.numpy as jnp
from jax import lax
from jax.experimental import pallas as pl
from jax.experimental.pallas import tpu as pltpu
from jax.sharding import PartitionSpec as P


f32, bf16, i32 = jnp.float32, jnp.bfloat16, jnp.int32
LIMIT = 40 * 1024 * 1024
FIRST_FLOPS = 20_000_000_000
MIX = 8
CONTRACT_ROWS = (((0,), (0,)), ((), ()))


def whole(space=pltpu.VMEM):
    return pl.BlockSpec(memory_space=space)


def spread_rows(row, rows):
    return jnp.broadcast_to(row, (rows, rows)).T


def one_hot(column, width):
    rows, lanes = column.shape
    lane = lax.broadcasted_iota(i32, (rows, lanes), 1)
    parts = [(column == lane + c).astype(bf16) for c in range(0, width, lanes)]
    return jnp.concatenate(parts, axis=1)


def mix(coef, basis, acc, begin, end):
    features = acc.shape[0]
    size, chunk = MIX, 32

    def body(g, _):
        at = begin + g * size
        factors = [coef[0, at + b] for b in range(size)]
        for start in range(0, features, chunk):
            part = pl.ds(start, chunk)
            total = acc[part, :]
            for b in range(size):
                total = total + factors[b] * basis[at + b, part, :].astype(f32)
            acc[part, :] = total
        return 0

    lax.fori_loop(0, (end - begin) // size, body, 0, unroll=True)


def send_kernel(n_dst, coef, mask, src, dst, table, weights, basis, _, messages, *rest):
    outs, acc = rest[:n_dst], rest[n_dst]
    count, _, cols = basis.shape
    blocks, block = src.shape[1:]
    per_owner = blocks // n_dst
    span = per_owner * block

    columns = [spread_rows(src[0, k : k + 1, :], block) for k in range(blocks)]
    picks = jnp.concatenate([one_hot(c, table.shape[0]) for c in columns], axis=0)
    picked = jnp.dot(picks, table[...], preferred_element_type=f32).astype(bf16)
    for k in range(blocks):
        scaled = weights[0, k] * mask[0, k].astype(f32).astype(bf16)
        messages[k * block : (k + 1) * block, :] = jnp.dot(
            scaled, picked[k * block : (k + 1) * block, :], preferred_element_type=f32
        ).astype(bf16)

    acc[...] = jnp.zeros_like(acc)
    mix(coef, basis, acc, 0, count)
    weight = acc[...].astype(bf16)
    me = lax.axis_index("dst")
    for d in range(n_dst):
        owner = me ^ d
        mine = messages[pl.ds(pl.multiple_of(owner * span, span), span), :]
        outs[d][:span, :] = jnp.dot(mine, weight, preferred_element_type=f32).astype(bf16)
        pad = outs[d].shape[0] - span
        which = lax.broadcasted_iota(i32, (pad, block), 0)
        slots = jnp.zeros((pad, block), i32)
        for b in range(per_owner):
            ids = dst[0, pl.ds(owner * per_owner + b, 1), :]
            slots = jnp.where(which == 2 * b, ids & 255, slots)
            slots = jnp.where(which == 2 * b + 1, ids >> 8, slots)
        outs[d][span:, :block] = slots.astype(f32).astype(bf16)
        outs[d][span:, block:] = jnp.zeros((pad, cols - block), bf16)


def send(coef, mask, src, dst, table, weights, basis, after, n_dst):
    features, cols = basis.shape[1:]
    blocks, block = src.shape[1:]
    span = blocks // n_dst * block
    pad = -(-2 * (blocks // n_dst) // 8) * 8
    return pl.pallas_call(
        functools.partial(send_kernel, n_dst),
        in_specs=[whole(pltpu.SMEM)] * 2 + [whole()] * 5 + [whole(pl.ANY)],
        out_shape=[jax.ShapeDtypeStruct((blocks * block, features), bf16)]
        + [jax.ShapeDtypeStruct((span + pad, cols), bf16)] * n_dst,
        out_specs=[whole()] * (1 + n_dst),
        scratch_shapes=[pltpu.VMEM((features, cols), f32)],
        compiler_params=pltpu.CompilerParams(vmem_limit_bytes=LIMIT),
        cost_estimate=pl.CostEstimate(flops=6_000_000_000, bytes_accessed=10_000_000, transcendentals=0),
        name="send",
    )(coef, mask, src, dst, table, weights, basis, after)


def first_kernel(out):
    out[...] = jnp.zeros_like(out)


def first():
    return pl.pallas_call(
        first_kernel,
        out_shape=jax.ShapeDtypeStruct((8, 128), f32),
        out_specs=whole(),
        compiler_params=pltpu.CompilerParams(vmem_limit_bytes=LIMIT),
        cost_estimate=pl.CostEstimate(flops=FIRST_FLOPS, bytes_accessed=4096, transcendentals=0),
        name="first",
    )()


def stack_kernel(_, *refs):
    parts, out = refs[:-1], refs[-1]
    rows_dev = parts[0].shape[0]
    for d, part in enumerate(parts):
        out[d * rows_dev : (d + 1) * rows_dev, :] = part[...]


def stack(after, parts):
    rows_dev, cols = parts[0].shape
    return pl.pallas_call(
        stack_kernel,
        in_specs=[whole(pl.ANY)] + [whole()] * len(parts),
        out_shape=jax.ShapeDtypeStruct((len(parts) * rows_dev, cols), bf16),
        out_specs=whole(),
        compiler_params=pltpu.CompilerParams(vmem_limit_bytes=LIMIT),
        name="stack",
    )(after, *parts)


def write_bias(type_rows, bias, added):
    rows_dev, cols = added.shape
    row = lax.broadcasted_iota(i32, (rows_dev, cols), 0) + lax.axis_index("rel") * rows_dev
    total = jnp.broadcast_to(bias[0:1, :], (rows_dev, cols))
    bound = 0
    for c in range(bias.shape[0] - 1):
        bound = bound + type_rows[c]
        total = jnp.where(row >= bound, bias[c + 1 : c + 2, :], total)
    added[...] = total


def outer_kernel(n_rel, n_dst, near, type_rows, bias, dst, messages, *rest):
    stacks, added, outer, late = rest[:near], rest[near], rest[near + 1], rest[near + 2 :]
    write_bias(type_rows, bias, added)
    blocks, block = dst.shape[1:]
    rows_dev = stacks[0].shape[0] // n_dst
    span = blocks // n_dst * block
    rel, me = lax.axis_index("rel"), lax.axis_index("dst")
    early = [[] for _ in range(near)]
    for d in range(n_dst):
        owner = me ^ d
        columns = [
            spread_rows(dst[0, pl.ds(owner * (span // block) + b, 1), :], block)
            for b in range(span // block)
        ]
        picks = jnp.concatenate(
            [
                jnp.concatenate(
                    [one_hot(c - (rel ^ e) * rows_dev, rows_dev) for e in range(n_rel)], axis=1
                )
                for c in columns
            ],
            axis=0,
        )
        summed = lax.dot_general(
            messages[pl.ds(pl.multiple_of(owner * span, span), span), :],
            picks,
            CONTRACT_ROWS,
            preferred_element_type=f32,
        ).astype(bf16)
        for e in range(n_rel):
            part = summed[:, e * rows_dev : (e + 1) * rows_dev]
            if e < near:
                early[e].append(part)
            else:
                late[e - near][:, d * rows_dev : (d + 1) * rows_dev] = part
    total = None
    for e in range(near):
        left = jnp.concatenate(early[e], axis=1)
        more = jnp.dot(left, stacks[e][...], preferred_element_type=f32)
        total = more if total is None else total + more
    outer[...] = total


def outer(type_rows, bias, dst, messages, stacks, n_rel, n_dst):
    features = messages.shape[1]
    rows, cols = stacks[0].shape
    near = len(stacks)
    return pl.pallas_call(
        functools.partial(outer_kernel, n_rel, n_dst, near),
        in_specs=[whole(pltpu.SMEM)] + [whole()] * (3 + near),
        out_shape=[
            jax.ShapeDtypeStruct((rows // n_dst, cols), f32),
            jax.ShapeDtypeStruct((features, cols), f32),
        ]
        + [jax.ShapeDtypeStruct((features, rows), bf16)] * (n_rel - near),
        out_specs=[whole()] * (2 + n_rel - near),
        compiler_params=pltpu.CompilerParams(vmem_limit_bytes=LIMIT),
        cost_estimate=pl.CostEstimate(flops=2_000_000_000, bytes_accessed=4_000_000, transcendentals=0),
        name="outer",
    )(type_rows, bias, dst, messages, *stacks)


def grad_kernel(count_late, basis, partial, *rest):
    lefts, rights = rest[:count_late], rest[count_late : 2 * count_late]
    out, outer, sums = rest[2 * count_late :]
    count, features, cols = basis.shape
    total = partial[...]
    for left, right in zip(lefts, rights):
        total = total + jnp.dot(left[...], right[...], preferred_element_type=f32)
    outer[...] = total.astype(bf16)

    size = 4

    def contract(g, _):
        totals = [jnp.zeros((8, 128), f32)] * size
        for start in range(0, features, 32):
            part = pl.ds(start, 32)
            side = outer[part, :]
            for b in range(size):
                prod = basis[g * size + b, part, :] * side
                more = (prod[:16, :] + prod[16:, :]).astype(f32)
                for r in range(0, 16, 8):
                    for c in range(0, cols, 128):
                        totals[b] = totals[b] + more[r : r + 8, c : c + 128]
        for b in range(size):
            sums[pl.ds(g * size + b, 1), :] = jnp.sum(totals[b], axis=0, keepdims=True)
        return 0

    lax.fori_loop(0, count // size, contract, 0, unroll=True)
    out[...] = jnp.sum(sums[...].T, axis=0, keepdims=True)


def grad(basis, partial, lefts, rights):
    features, cols = basis.shape[1:]
    return pl.pallas_call(
        functools.partial(grad_kernel, len(lefts)),
        in_specs=[whole()] * (2 + 2 * len(lefts)),
        out_shape=jax.ShapeDtypeStruct((1, 128), f32),
        out_specs=whole(),
        scratch_shapes=[pltpu.VMEM((features, cols), bf16), pltpu.VMEM((128, 128), f32)],
        compiler_params=pltpu.CompilerParams(vmem_limit_bytes=LIMIT),
        cost_estimate=pl.CostEstimate(flops=4_000_000_000, bytes_accessed=10_000_000, transcendentals=0),
        name="grad",
    )(basis, partial, *lefts, *rights)


def gather_kernel(n_rel, n_dst, block, added, *refs):
    got, outs = refs[:n_dst], refs[n_dst:]
    rows_dev = outs[0].shape[0]
    span = got[0].shape[0] // block * block
    rel = lax.axis_index("rel")
    ids = []
    for d in range(n_dst):
        pairs = got[d][span:, :block].astype(f32)
        ids.append(
            [
                (pairs[2 * b : 2 * b + 1] + 256.0 * pairs[2 * b + 1 : 2 * b + 2]).astype(i32)
                for b in range(span // block)
            ]
        )
    row = lax.broadcasted_iota(i32, (rows_dev, block), 0)
    for e in range(n_rel):
        place = row + (rel ^ e) * rows_dev
        total = None
        for d in range(n_dst):
            picks = jnp.concatenate(
                [(place == one).astype(bf16) for one in ids[d]], axis=1
            )
            more = jnp.dot(picks, got[d][:span, :], preferred_element_type=f32)
            total = more if total is None else total + more
        if e == 0:
            total = total + added[...]
        outs[e][...] = total.astype(outs[e].dtype)


def gather(added, got, n_rel, block, rows_dev):
    n_dst, cols = len(got), got[0].shape[1]
    return pl.pallas_call(
        functools.partial(gather_kernel, n_rel, n_dst, block),
        in_specs=[whole()] * (1 + n_dst),
        out_shape=[
            jax.ShapeDtypeStruct((rows_dev, cols), f32 if e == 0 else bf16)
            for e in range(n_rel)
        ],
        out_specs=[whole()] * n_rel,
        compiler_params=pltpu.CompilerParams(vmem_limit_bytes=LIMIT),
        cost_estimate=pl.CostEstimate(flops=600_000_000, bytes_accessed=1_000_000, transcendentals=0),
        name="gather",
    )(added, *got)


def finish_kernel(*refs):
    parts, out = refs[:-1], refs[-1]
    total = parts[0][...]
    for part in parts[1:]:
        total = total + part[...].astype(f32)
    out[...] = total.astype(out.dtype)


def finish(parts):
    return pl.pallas_call(
        finish_kernel,
        in_specs=[whole()] * len(parts),
        out_shape=jax.ShapeDtypeStruct(parts[0].shape, bf16),
        out_specs=whole(),
        compiler_params=pltpu.CompilerParams(vmem_limit_bytes=LIMIT),
        name="finish",
    )(*parts)


def on_device(
    node_table,
    edge_weights,
    src_ids,
    dst_ids,
    block_mask,
    basis_coef,
    basis_mats,
    type_bias,
    type_rows,
    cotangent,
):
    n_rel, n_dst, n_mp = (lax.axis_size(a) for a in ("rel", "dst", "mp"))
    block = edge_weights.shape[-1]
    rows_dev = cotangent.shape[0]

    def swap(x, axis, d):
        n = lax.axis_size(axis)
        return lax.ppermute(x, axis, [(i, i ^ d) for i in range(n)])

    along = [cotangent] + [swap(cotangent, "dst", d) for d in range(1, n_dst)]
    begun = first()
    messages, *queues = send(
        basis_coef,
        block_mask,
        src_ids,
        dst_ids,
        node_table,
        edge_weights,
        basis_mats,
        begun,
        n_dst,
    )
    got = [queues[0]] + [swap(queues[d], "dst", d) for d in range(1, n_dst)]
    stacked = stack(messages, along)

    stacks = [None] * n_rel
    for e in range(0, n_rel, 2):
        stacks[e] = swap(stacked, "rel", e) if e else stacked
        stacks[e + 1] = swap(stacks[e], "rel", 1)
    added, outer_sum, *lefts = outer(
        type_rows, type_bias, dst_ids, messages, stacks[:2], n_rel, n_dst
    )
    partial = grad(basis_mats, outer_sum, lefts, stacks[2:])

    sums = gather(added, got, n_rel, block, rows_dev)
    parts = [sums[0]] + [swap(sums[e], "rel", e) for e in range(1, n_rel)]
    layer_out = finish(parts)

    for axis, size in (("mp", n_mp), ("dst", n_dst)):
        d = 1
        while d < size:
            partial = partial + swap(partial, axis, d)
            d *= 2
    return layer_out, partial[:, : basis_coef.shape[1]]


def solution(mesh):
    in_specs = (
        P(("rel", "dst"), None),
        P("rel", "dst", None, None),
        P("rel", "dst", None),
        P("rel", "dst", None),
        P("rel", "dst"),
        P("rel", None),
        P(None, None, "mp"),
        P(None, "mp"),
        P(),
        P(("rel", "dst"), "mp"),
    )
    out_specs = (P(("rel", "dst"), "mp"), P("rel", None))

    return jax.shard_map(
        on_device, mesh=mesh, in_specs=in_specs, out_specs=out_specs, check_vma=False
    )
```
